32 devices in a mesh: expert: 4 (over z), mp: 8 (over y, x, core).
Axes of the slice: x: 2, y: 2, z: 4, core: 2. Of those that a mesh axis runs over, the one named last changes fastest.
Arguments:
- tokens: bfloat16 [512, 4096], P(('expert', 'mp')), may hold values from -6 to 6
- gain: bfloat16 [4096], replicated, may hold values from 0.5 to 1.5
- expert_ids: int32 [512, 2], P(('expert', 'mp')), may hold values from 0 to 3, all different within a row; in each aligned block of 16 rows (0 to 15, 16 to 31, ...) at most 10 rows name the same one
- gate_num: int32 [512], P(('expert', 'mp')), may hold values from 1 to 1023
- w_gate: bfloat16 [4, 4096, 14336], P('expert', None, 'mp'), may hold values from -0.09375 to 0.09375
- w_up: bfloat16 [4, 4096, 14336], P('expert', None, 'mp'), may hold values from -0.09375 to 0.09375
- w_down: bfloat16 [4, 14336, 4096], P('expert', 'mp'), may hold values from -0.046875 to 0.046875
Outputs:
- mixed_out: bfloat16 [512, 4096], P(('expert', 'mp'))
The draws below stay inside these ranges and needn't reach their ends.
Inputs may be any that keep to these rules, and one draw needn't show every extreme that they name: `expert_ids`: the 2 ids of a token differ. Within the rows of one device no expert is named more than 10 times, and some expert reaches 10 on some devices.
All inputs are finite; a program needn't handle non-finite values.
Results may differ from the reference program's by a relative error of at most 0.019.
Values may be sent and summed in bfloat16 or wider, within the bound.
No kernel may reach another device: no remote copies, remote signals or barrier semaphores. Data moves between devices by JAX's collectives and lax.ppermute only.
A program may use at most 128 MiB of HBM per device.

```python
import math
import jax
import jax.numpy as jnp
import numpy as np
from jax import lax

D = 4096
FF = 14336
TOP = 2
DENOM = 1024
TOK_DEV = 16
EXPERTS = 4
TOKENS = 512
CAP = 10
ROWS_MAX = 320
FF_SHARD = 1792
N_MP = 8


def plant(values, rng, low, high):
    extent = values.shape
    index_at = [jax.random.randint(jax.random.fold_in(rng, axis), (), 0, extent[axis]) for axis in range(len(extent))]
    values = values.at[tuple(index_at)].set(low)
    longest = extent.index(max(extent))
    index_at[longest] = (index_at[longest] + 1) % extent[longest]
    return values.at[tuple(index_at)].set(high)


def shard_levels(rng, shape, pieces, least, largest):
    loudness, own = 1.0, jax.random.fold_in(rng, 6)
    for position, blocks in pieces:
        steps = jnp.exp(jax.random.uniform(jax.random.fold_in(own, position), (blocks,), jnp.float32, least / len(pieces), largest / len(pieces)))
        loudness = loudness * jnp.repeat(steps, shape[position] // blocks).reshape([-1 if axis == position else 1 for axis in range(len(shape))])
    return loudness


def assign_block(own_key, own, number, rows, count, top, most, lean):
    order = jax.random.permutation(own_key, count)
    heavy_load, common = shares(count, rows * top, most, lean, True), shares(count, rows * top, most, lean, False)
    places = jnp.arange(count)

    def named(lengths, rotation):
        used = int((lengths > 0).sum())
        fixed = max(1, used // 4)
        moved = fixed + (places - fixed + rotation * (used - fixed)) % max(1, count - fixed)
        return jnp.zeros((count,), jnp.int32).at[order[jnp.where(places < fixed, places, moved)]].set(jnp.asarray(lengths, jnp.int32))

    lengths = jnp.where(number % 4 == 0, named(heavy_load, number // 4), named(common, number - number // 4 - 1))
    mixed = jax.random.permutation(jax.random.fold_in(own, 3), count)
    source_of, taker = mixed[0:count // 2 * 2:2], mixed[1:count // 2 * 2:2]
    margin = jnp.minimum(lengths[source_of] - 1, most - lengths[taker]) // 2
    margin = jnp.where((source_of == order[0]) | (taker == order[0]) | (lengths[taker] == 0), 0, jnp.maximum(margin, 0))
    moved = jax.random.randint(jax.random.fold_in(own, 4), (count // 2,), 0, 1 << 20) % (margin + 1)
    lengths = lengths.at[source_of].add(-moved).at[taker].add(moved)
    labels = jnp.searchsorted(jnp.cumsum(lengths), jnp.arange(rows * top), side="right").astype(jnp.int32)
    grid = labels.reshape(top, rows).T
    grid = grid[jax.random.permutation(jax.random.fold_in(own, 1), rows)]
    rotation = jax.random.randint(jax.random.fold_in(own, 2), (rows, 1), 0, top)
    return jnp.take_along_axis(grid, (jnp.arange(top)[None, :] + rotation) % top, axis=1)


def shares(number_of, total, reach, skew, full):
    portions = [(1 << 20) // math.isqrt(grade ** skew) + 1 for grade in range(1, number_of + 1)]
    largest = reach if full else min(reach, max(-(-total // number_of), total * portions[0] // sum(portions)))
    least = 1 if total - largest >= number_of - 1 else 0
    counts, spare = [largest] + [least] * (number_of - 1), total - largest - least * (number_of - 1)
    while spare > 0:
        candidates = [i for i in range(1, number_of) if counts[i] < largest] or [i for i in range(1, number_of) if counts[i] < reach]
        whole, budget = sum([portions[i] for i in candidates]), spare
        for i in candidates:
            extra = min(reach - counts[i], max(1, budget * portions[i] // whole), spare)
            counts[i] = counts[i] + extra
            spare = spare - extra
    return np.array(counts)


def bell_draw(stream_key, shape, spread, most, shards=(), kind=jnp.bfloat16):
    values = jax.random.normal(stream_key, shape, jnp.float32) * spread
    if len(shards) > 0:
        values = shard_levels(stream_key, shape, shards, -0.22, 0.18) * values
    return jnp.clip(values, min=-most, max=most).astype(kind)


def setup_inputs(seed: int = 0) -> dict:
    keys = jax.random.split(jax.random.key(seed), 8)
    tokens = bell_draw(keys[0], (TOKENS, D), 1.0, 6.0, ((0, 32),))
    gain = jnp.clip(1.0 + 0.1 * jax.random.normal(keys[1], (D,), jnp.float32), 0.5, 1.5).astype(jnp.bfloat16)
    expert_ids_keys = jax.random.split(jax.random.fold_in(keys[2], 1), TOKENS // TOK_DEV)
    expert_ids_turns = jax.random.permutation(jax.random.fold_in(keys[2], 3), TOKENS // TOK_DEV)
    expert_ids = jax.vmap(lambda own, number: assign_block(jax.random.fold_in(keys[2], 2), own, number, TOK_DEV, EXPERTS, TOP, CAP, 2))(expert_ids_keys, expert_ids_turns).reshape((TOKENS, TOP))
    gate_num = plant(jax.random.randint(keys[3], (TOKENS,), 1, DENOM), jax.random.fold_in(keys[3], 1), 1, DENOM - 1).astype(jnp.int32)
    w_gate = bell_draw(keys[4], (EXPERTS, D, FF), D ** -0.5, 0.09375, ((0, 4), (2, 8)))
    w_up = bell_draw(keys[5], (EXPERTS, D, FF), D ** -0.5, 0.09375, ((0, 4), (2, 8)))
    w_down = bell_draw(keys[6], (EXPERTS, FF, D), FF ** -0.5, 0.046875, ((0, 4), (1, 8)))
    return dict(tokens=tokens, gain=gain, expert_ids=expert_ids, gate_num=gate_num, w_gate=w_gate, w_up=w_up, w_down=w_down)


def rms_normed(tokens, gain):
    values = tokens.astype(jnp.float32)
    inverse = lax.rsqrt(lax.optimization_barrier(jnp.mean(values * values, axis=1, keepdims=True)) + 1e-05)
    return (values * inverse * gain.astype(jnp.float32)).astype(jnp.bfloat16)

def swiglu(row_block, gate_matrix, up_matrix):
    gate_proj = jnp.dot(row_block, gate_matrix, preferred_element_type=jnp.float32)
    up_proj = jnp.dot(row_block, up_matrix, preferred_element_type=jnp.float32)
    return (jax.nn.silu(gate_proj) * up_proj).astype(jnp.bfloat16)

def reference(tokens, gain, expert_ids, gate_num, w_gate, w_up, w_down):
    normed = rms_normed(tokens, gain)
    flat_ids = expert_ids.reshape(-1).astype(jnp.int32)
    first_share = gate_num.astype(jnp.float32) / DENOM
    weights = jnp.stack([first_share, 1.0 - first_share], axis=1).reshape(-1)

    def one_expert(expert):
        off_expert = (flat_ids != expert).astype(jnp.int32)
        slot_order = jnp.argsort(off_expert, stable=True)[:ROWS_MAX].astype(jnp.int32)
        filled = flat_ids[slot_order] == expert
        token_rows = (slot_order // TOP).astype(jnp.int32)
        row_block = jnp.take(normed, token_rows, axis=0)
        row_block = jnp.where(filled[:, None], row_block, jnp.zeros_like(row_block))
        hidden = swiglu(row_block, w_gate[expert], w_up[expert])
        hidden_groups = hidden.reshape(ROWS_MAX, N_MP, FF_SHARD).transpose(1, 0, 2)
        down_rows = w_down[expert].reshape(N_MP, FF_SHARD, D)

        def add_group(running, group_pair):
            group_part = jnp.dot(group_pair[0], group_pair[1], preferred_element_type=jnp.float32).astype(jnp.bfloat16)
            group_part = lax.optimization_barrier(group_part)
            return (running + group_part.astype(jnp.float32), None)
        running, _ = lax.scan(add_group, jnp.zeros((ROWS_MAX, D), jnp.float32), (hidden_groups, down_rows))
        result = lax.optimization_barrier(running.astype(jnp.bfloat16)).astype(jnp.float32)
        slot_weight = jnp.where(filled, weights[slot_order], jnp.float32(0.0))
        return (result * slot_weight[:, None], token_rows)
    scaled, token_index = lax.map(one_expert, jnp.arange(EXPERTS, dtype=jnp.int32))
    mixed_out = jnp.zeros((TOKENS, D), jnp.float32).at[token_index.reshape(-1)].add(scaled.reshape(-1, D))
    return mixed_out.astype(jnp.bfloat16)
```

```python
import functools
import math

import jax
import jax.numpy as jnp
from jax import lax
from jax.experimental import pallas as pl
from jax.experimental.pallas import tpu as pltpu
from jax.sharding import PartitionSpec as P

DENOM = 1024
CHUNKS = 2
MIB = 1 << 20


def f32dot(a, b):
    return jnp.dot(a, b, preferred_element_type=jnp.float32)


def call(kernel, out_shape, vmem_mib, **kw):
    return pl.pallas_call(
        kernel,
        out_shape=out_shape,
        compiler_params=pltpu.CompilerParams(vmem_limit_bytes=vmem_mib * MIB),
        **kw,
    )


def vspec():
    return pl.BlockSpec(memory_space=pltpu.VMEM)


def slot_match(ids, me, groups, cap, pieces):
    tok = ids.shape[1]
    rows = groups * pieces * cap
    r = lax.broadcasted_iota(jnp.int32, (rows, tok), 0)
    block = r // (pieces * cap)
    piece = (r // cap) % pieces
    place = r % cap
    expert = (me + block) % groups
    first = ids[0:1, :] == expert
    second = ids[1:2, :] == expert
    named = jnp.where(first | second, 1.0, 0.0)
    a = lax.broadcasted_iota(jnp.int32, (tok, tok), 0)
    b = lax.broadcasted_iota(jnp.int32, (tok, tok), 1)
    before = jnp.where(a < b, 1.0, 0.0).astype(jnp.bfloat16)
    position = f32dot(named.astype(jnp.bfloat16), before)
    here = position == place.astype(jnp.float32)
    return here & first, here & second, piece


def pack_kernel(me, tokens, gain, ids, *outs, groups, cap, pieces):
    values = tokens[...].astype(jnp.float32)
    inverse = lax.rsqrt(jnp.mean(values * values, axis=1, keepdims=True) + 1e-05)
    normed = (values * inverse * gain[...].astype(jnp.float32)).astype(jnp.bfloat16)
    s0, s1, piece = slot_match(ids[...], me[0], groups, cap, pieces)
    hit = s0 | s1
    chunks = len(outs) // groups
    width = tokens.shape[1] // chunks // pieces
    rows = pieces * cap
    sel = [
        jnp.where(hit & (piece == g), 1.0, 0.0).astype(jnp.bfloat16) for g in range(pieces)
    ]
    for c in range(chunks):
        acc = 0.0
        for g in range(pieces):
            at = (c * pieces + g) * width
            acc += f32dot(sel[g], normed[:, at : at + width])
        acc = acc.astype(jnp.bfloat16)
        for j in range(groups):
            outs[c * groups + j][...] = acc[j * rows : (j + 1) * rows]


def unpack_kernel(*refs, cap, pieces):
    blocks, out = refs[:-1], refs[-1]
    rows, width = blocks[0].shape
    slots = len(blocks) * cap
    s = lax.broadcasted_iota(jnp.int32, (slots, rows), 0)
    r = lax.broadcasted_iota(jnp.int32, (slots, rows), 1)
    for g in range(pieces):
        acc = 0.0
        for j, block in enumerate(blocks):
            pick = (s - j * cap == r - g * cap) & (s // cap == j)
            acc += f32dot(jnp.where(pick, 1.0, 0.0).astype(jnp.bfloat16), block[...])
        out[:, g * width : (g + 1) * width] = acc.astype(jnp.bfloat16)


def up_kernel(*refs, parts, first, last):
    xs, rest = refs[:parts], refs[parts:]
    w_gate, w_up = rest[0], rest[1]
    rest = rest[2:]
    if not first:
        old_gate, old_up = rest[0], rest[1]
        rest = rest[2:]
    outs, x = rest[:-1], rest[-1]

    @pl.when(pl.program_id(0) == 0)
    def _():
        at = 0
        for part in xs:
            x[at : at + part.shape[0]] = part[...]
            at += part.shape[0]

    gate = f32dot(x[...], w_gate[...])
    up = f32dot(x[...], w_up[...])
    if not first:
        gate += old_gate[...]
        up += old_up[...]
    if last:
        outs[0][...] = (gate / (1.0 + jnp.exp(-gate)) * up).astype(jnp.bfloat16)
    else:
        outs[0][...] = gate
        outs[1][...] = up


def down_kernel(hidden, w_down, mine, theirs):
    half = mine.shape[0]
    part = f32dot(hidden[...], w_down[...]).astype(jnp.bfloat16)
    mine[...] = part[:half]
    theirs[...] = part[half:]


def core_sum_kernel(mine, got, *outs):
    total = (mine[...].astype(jnp.float32) + got[...].astype(jnp.float32)).astype(jnp.bfloat16)
    rows = outs[0].shape[0]
    for i, out in enumerate(outs):
        out[...] = total[i * rows : (i + 1) * rows]


def chip_sum_kernel(*refs, parts, cap, pieces):
    ins, outs = refs[:parts], refs[parts:]
    total = ins[0][...].astype(jnp.float32)
    for ref in ins[1:]:
        total += ref[...].astype(jnp.float32)
    total = total.astype(jnp.bfloat16)
    rows, width = outs[0].shape
    slots = total.shape[0]
    r = lax.broadcasted_iota(jnp.int32, (len(outs) * rows, slots), 0)
    s = lax.broadcasted_iota(jnp.int32, (len(outs) * rows, slots), 1)
    block, piece, place = r // rows, (r // cap) % pieces, r % cap
    hit = s == block * cap + place
    acc = 0.0
    for g in range(pieces):
        pick = jnp.where(hit & (piece == g), 1.0, 0.0).astype(jnp.bfloat16)
        acc += f32dot(pick, total[:, g * width : (g + 1) * width])
    acc = acc.astype(jnp.bfloat16)
    for j, out in enumerate(outs):
        out[...] = acc[j * rows : (j + 1) * rows]


def mix_kernel(me, ids, gate_num, *refs, groups, cap, pieces):
    blocks, out = refs[:-1], refs[-1]
    chunks = len(blocks) // groups
    rows, width = blocks[0].shape
    s0, s1, piece = slot_match(ids[...], me[0], groups, cap, pieces)
    tok = out.shape[0]
    share = gate_num[...].astype(jnp.float32) / DENOM
    a = lax.broadcasted_iota(jnp.int32, (tok, tok), 0)
    b = lax.broadcasted_iota(jnp.int32, (tok, tok), 1)
    share = jnp.sum(jnp.where(a == b, share, 0.0), axis=1, keepdims=True)
    turned = (((0,), (0,)), ((), ()))
    for g in range(pieces):
        pick0 = jnp.where(s0 & (piece == g), 1.0, 0.0).astype(jnp.bfloat16)
        pick1 = jnp.where(s1 & (piece == g), 1.0, 0.0).astype(jnp.bfloat16)
        for c in range(chunks):
            c0 = c1 = 0.0
            for j in range(groups):
                block = blocks[c * groups + j][...]
                at = slice(j * rows, (j + 1) * rows)
                c0 += lax.dot_general(pick0[at], block, turned, preferred_element_type=jnp.float32)
                c1 += lax.dot_general(pick1[at], block, turned, preferred_element_type=jnp.float32)
            at = (c * pieces + g) * width
            out[:, at : at + width] = (c0 * share + c1 * (1.0 - share)).astype(jnp.bfloat16)


def tile_of(size, most):
    return max([t for t in range(128, most + 1, 128) if size % t == 0], default=size)


def body(tokens, gain, expert_ids, gate_num, w_gate, w_up, w_down):
    groups, members = lax.axis_size("expert"), lax.axis_size("mp")
    tok, width = tokens.shape
    top = expert_ids.shape[1]
    hid = w_gate.shape[2]
    cap = (5 * tok * top + 4 * groups - 1) // (4 * groups)
    pieces = 8 // math.gcd(cap, 8)
    chunks = CHUNKS
    cols = width // chunks
    thin = cols // pieces
    slots = groups * cap
    rows = members * slots
    offsets = list(range(0, members, 2))
    bf16 = jnp.bfloat16
    me = lax.axis_index("expert").astype(jnp.int32).reshape(1)
    ids = expert_ids.T
    smem = pl.BlockSpec(memory_space=pltpu.SMEM)

    def swap(value, bit):
        return lax.ppermute(value, "mp", [(i, i ^ bit) for i in range(members)])

    def shift(value, by):
        return lax.ppermute(value, "expert", [(i, (i + by) % groups) for i in range(groups)])

    shape = functools.partial(jax.ShapeDtypeStruct, dtype=bf16)
    packed = call(
        functools.partial(pack_kernel, groups=groups, cap=cap, pieces=pieces),
        [shape((pieces * cap, thin))] * (groups * chunks),
        8,
        in_specs=[smem, vspec(), vspec(), vspec()],
        name="pack",
    )(me, tokens, gain.reshape(1, -1), ids)

    gate = up = hidden = None
    tile = tile_of(hid, 256)
    for c in range(chunks):
        blocks = packed[c * groups : (c + 1) * groups]
        got = [blocks[0]] + [shift(blocks[j], j) for j in range(1, groups)]
        own = call(
            functools.partial(unpack_kernel, cap=cap, pieces=pieces),
            shape((slots, cols)),
            8,
            name="unpack",
        )(*got)
        near = [own] + [swap(own, bit) for bit in offsets[1:]]
        xs = near + [swap(v, 1) for v in near]
        first, last = c == 0, c == chunks - 1
        full = [pl.BlockSpec((slots, cols), lambda n: (0, 0))] * members
        weight = pl.BlockSpec((None, cols, tile), lambda n, c=c: (0, c, n))
        part = pl.BlockSpec((rows, tile), lambda n: (0, n))
        args = xs + [w_gate, w_up] + ([] if first else [gate, up])
        result = call(
            functools.partial(up_kernel, parts=members, first=first, last=last),
            [shape((rows, hid))]
            if last
            else [jax.ShapeDtypeStruct((rows, hid), jnp.float32)] * 2,
            32,
            grid=(hid // tile,),
            in_specs=full + [weight] * 2 + ([] if first else [part] * 2),
            out_specs=[part] if last else [part] * 2,
            scratch_shapes=[pltpu.VMEM((rows, cols), bf16)],
            name="up",
            cost_estimate=pl.CostEstimate(
                flops=4 * rows * cols * hid, transcendentals=0, bytes_accessed=4 * cols * hid
            ),
        )(*args)
        if last:
            hidden = result[0]
        else:
            gate, up = result

    tile = tile_of(cols, 512)
    back = []
    for c in range(chunks):
        mine, theirs = call(
            down_kernel,
            [shape((rows // 2, cols))] * 2,
            24,
            grid=(cols // tile,),
            in_specs=[
                pl.BlockSpec((rows, hid), lambda n: (0, 0)),
                pl.BlockSpec((None, hid, tile), lambda n, c=c: (0, 0, c * (cols // tile) + n)),
            ],
            out_specs=[pl.BlockSpec((rows // 2, tile), lambda n: (0, n))] * 2,
            name="down",
            cost_estimate=pl.CostEstimate(
                flops=2 * rows * cols * hid, transcendentals=0, bytes_accessed=2 * cols * hid
            ),
        )(hidden, w_down)
        sums = call(
            core_sum_kernel, [shape((slots, cols))] * len(offsets), 16, name="core_sum"
        )(mine, swap(theirs, 1))
        near = [sums[0]] + [swap(v, bit) for v, bit in zip(sums[1:], offsets[1:])]
        blocks = call(
            functools.partial(chip_sum_kernel, parts=len(near), cap=cap, pieces=pieces),
            [shape((pieces * cap, thin))] * groups,
            16,
            name="chip_sum",
        )(*near)
        back += [blocks[0]] + [shift(blocks[j], -j) for j in range(1, groups)]

    return call(
        functools.partial(mix_kernel, groups=groups, cap=cap, pieces=pieces),
        shape((tok, width)),
        16,
        in_specs=[smem] + [vspec()] * (2 + len(back)),
        name="mix",
    )(me, ids, gate_num.reshape(1, -1), *back)


def solution(mesh):
    in_specs = (
        P(("expert", "mp"), None),
        P(),
        P(("expert", "mp"), None),
        P(("expert", "mp")),
        P("expert", None, "mp"),
        P("expert", None, "mp"),
        P("expert", "mp", None),
    )
    out_specs = P(("expert", "mp"), None)
    return jax.shard_map(body, mesh=mesh, in_specs=in_specs, out_specs=out_specs, check_vma=False)
```
